32 devices in a mesh: dev: 8 (over z, x), rep: 4 (over y, core).
Axes of the slice: x: 2, y: 2, z: 4, core: 2. Of those that a mesh axis runs over, the one named last changes fastest.
Arguments:
- h_zero: bfloat16 [32768, 256], P(('dev', 'rep')), may hold values from 0 to 2
- h_prev: bfloat16 [32768, 256], P(('dev', 'rep')), may hold values from 0 to 2
- hist_a: bfloat16 [32768, 256], P('dev'), may hold values from 0 to 2
- hist_b: bfloat16 [32768, 256], P('dev'), may hold values from 0 to 2
- tile_vals: bfloat16 [256, 12, 128, 128], P(('dev', 'rep'))
- tile_cols: int32 [256, 12], P(('dev', 'rep')), may hold values from 0 to 47, as said below
- pull_rows: int32 [32, 8, 128], P(('dev', 'rep')), may hold values from 0 to 4095
- pull_counts: int32 [32, 8], P(('dev', 'rep')), may hold values from 96 to 128, as said below
- weight_two: bfloat16 [256, 256], replicated, may hold values from -0.375 to 0.375
- weight_three: bfloat16 [256, 256], replicated, may hold values from -0.375 to 0.375
- grad_out: bfloat16 [32768, 256], P(('dev', 'rep')), may hold values from -0.125 to 0.125
Outputs:
- layer_three: bfloat16 [32768, 256], P(('dev', 'rep'))
- new_history: bfloat16 [32768, 256], P('dev')
- weight_grad: float32 [256, 256], replicated
The draws below stay inside these ranges and needn't reach their ends.
Inputs may be any that keep to these rules, and one draw needn't show every extreme that they name: `tile_cols`: entry 0 of a row block names one of its device's own 8 blocks; entries 1 to 3 name blocks of the owner's history shard; the other 8 name pulled blocks of consecutive owners modulo 8, and every owner's block is named by some row block of each device. `pull_rows`: entries at slots at or past the block's count are read by no output. `pull_counts`: every device pulls a full block of 128 rows from some owner and a block of exactly 96 rows from another.
All inputs are finite; a program needn't handle non-finite values.
Results may differ from the reference program's by a relative error of at most 0.0034.
Values may be sent and summed in bfloat16 or wider, within the bound.
No kernel may reach another device: no remote copies, remote signals or barrier semaphores. Data moves between devices by JAX's collectives and lax.ppermute only.
A program may use at most 128 MiB of HBM per device.

```python
import math
import jax
import jax.numpy as jnp
from jax import lax

WIDTH = 256
BATCH = 1024
TILE = 128
HOME_TILES = 3
REMOTE_TILES = 8
TPR = 12
ROWBLK = 8
WORKERS = 32
SHARD = 4096
NODES = 32768
N_DEV = 8
N_REP = 4


def draw_tile_vals(key, part):
    full_shape = (WORKERS * ROWBLK, TPR, TILE, TILE)
    key_mask, key_value = jax.random.split(key, 2)
    edge_mask = jax.random.bernoulli(key_mask, 0.125, full_shape).astype(jnp.float32)
    edge_weight = jax.random.uniform(key_value, full_shape, jnp.float32, 0.5, 1.5)
    return (edge_mask * edge_weight * (8.0 / (TPR * TILE))).astype(jnp.bfloat16)


def draw_tile_cols(key, part):
    key_local, key_home, key_shift = jax.random.split(key, 3)
    row_count = WORKERS * ROWBLK
    local_cols = jax.random.randint(key_local, (row_count, 1), 0, ROWBLK, jnp.int32)
    home_cols = jax.random.randint(key_home, (row_count, HOME_TILES), ROWBLK, ROWBLK + N_REP * ROWBLK, jnp.int32)
    shifts = jax.random.randint(key_shift, (WORKERS, 1), 0, N_DEV, jnp.int32)
    shift_rows = jnp.repeat(shifts, ROWBLK, axis=0)
    block_pos = (jnp.arange(row_count, dtype=jnp.int32) % ROWBLK)[:, None]
    slot_pos = jnp.arange(REMOTE_TILES, dtype=jnp.int32)[None, :]
    peer_ids = (block_pos * REMOTE_TILES + slot_pos + shift_rows) % N_DEV
    remote_cols = ROWBLK + N_REP * ROWBLK + peer_ids
    return jnp.concatenate([local_cols, home_cols, remote_cols], axis=1).astype(jnp.int32)


def draw_pull_counts(key, part):
    key_one, key_two, key_full = jax.random.split(key, 3)
    full_shape = (WORKERS, N_DEV)
    first = jax.random.randint(key_one, full_shape, 1, TILE + 1, jnp.int32)
    second = jax.random.randint(key_two, full_shape, 1, TILE + 1, jnp.int32)
    counts = TILE - first * second // (4 * TILE)
    offset = jax.random.randint(key_full, (), 0, N_DEV, jnp.int32)
    full_peer = (jnp.arange(WORKERS, dtype=jnp.int32) * 5 + offset) % N_DEV
    low_peer = (full_peer + 1) % N_DEV
    peer_ids = jnp.arange(N_DEV, dtype=jnp.int32)[None, :]
    counts = jnp.where(peer_ids == low_peer[:, None], TILE - TILE // 4, counts)
    counts = jnp.where(peer_ids == full_peer[:, None], TILE, counts)
    return counts.astype(jnp.int32)


def set_ends(drawn, stream_key, low, top_value):
    spot = [jax.random.randint(jax.random.fold_in(stream_key, axis), (), 0, length) for axis, length in enumerate(drawn.shape)]
    longest = drawn.shape.index(max(drawn.shape))
    next_to = spot[:longest] + [(spot[longest] + 1) % drawn.shape[longest]] + spot[longest + 1:]
    return drawn.at[tuple(spot)].set(low).at[tuple(next_to)].set(top_value)


def levels(rng, dims, cuts, low, top_value):
    gain = 1.0
    for axis_at, parts in cuts:
        draws = jax.random.uniform(jax.random.fold_in(jax.random.fold_in(rng, 6), axis_at), (parts,), jnp.float32, low / len(cuts), top_value / len(cuts))
        gain = gain * jnp.repeat(jnp.exp(draws), dims[axis_at] // parts).reshape((-1,) + (1,) * (len(dims) - 1 - axis_at))
    return gain


def gaussian(key, extent, spread, most, pieces=(), kind=jnp.bfloat16):
    level = levels(key, extent, pieces, -0.22, 0.18) if pieces else 1.0
    entries = jax.random.normal(key, extent, jnp.float32) * spread * level
    return jnp.minimum(jnp.maximum(entries, -most), most).astype(kind)


def setup_inputs(seed: int = 0) -> dict:
    key_list = jax.random.split(jax.random.key(seed), 12)
    return {
        "h_zero": jnp.clip(2.0 * jax.random.uniform(key_list[0], (NODES, WIDTH), jnp.float32) ** levels(key_list[0], (NODES, WIDTH), ((0, 32),), -0.2, 0.2), 0.0, 2.0).astype(jnp.bfloat16),
        "h_prev": jnp.clip(2.0 * jax.random.uniform(key_list[1], (NODES, WIDTH), jnp.float32) ** levels(key_list[1], (NODES, WIDTH), ((0, 32),), -0.2, 0.2), 0.0, 2.0).astype(jnp.bfloat16),
        "hist_a": jnp.clip(2.0 * jax.random.uniform(key_list[2], (NODES, WIDTH), jnp.float32) ** levels(key_list[2], (NODES, WIDTH), ((0, 8),), -0.2, 0.2), 0.0, 2.0).astype(jnp.bfloat16),
        "hist_b": jnp.clip(2.0 * jax.random.uniform(key_list[3], (NODES, WIDTH), jnp.float32) ** levels(key_list[3], (NODES, WIDTH), ((0, 8),), -0.2, 0.2), 0.0, 2.0).astype(jnp.bfloat16),
        "tile_vals": draw_tile_vals(jax.random.fold_in(key_list[11], 71), 0),
        "tile_cols": draw_tile_cols(jax.random.fold_in(key_list[11], 71), 0),
        "pull_rows": set_ends(jax.random.randint(key_list[6], (WORKERS, N_DEV, TILE), 0, SHARD), jax.random.fold_in(key_list[6], 1), 0, SHARD - 1).astype(jnp.int32),
        "pull_counts": draw_pull_counts(jax.random.fold_in(key_list[11], 71), 0),
        "weight_two": gaussian(key_list[8], (WIDTH, WIDTH), WIDTH ** -0.5, 0.375),
        "weight_three": gaussian(key_list[9], (WIDTH, WIDTH), WIDTH ** -0.5, 0.375),
        "grad_out": gaussian(key_list[10], (NODES, WIDTH), (4.0 / NODES ** 0.5), 0.125, ((0, 32),)),
    }


restart = 0.1
strength = 0.5


def propagate(current, history, pulled, values, columns, start_rows, weight, layer_number):
    feature_width = current.shape[1]
    source = jnp.concatenate([current, history, pulled.reshape(-1, feature_width)], axis=0)
    blocks = source.reshape(-1, TILE, feature_width)
    picked = jnp.take(blocks, columns.reshape(-1), axis=0).reshape(columns.shape + (TILE, feature_width))
    summed = jnp.einsum("btij,btjf->bif", values.astype(jnp.float32), picked.astype(jnp.float32))
    summed = summed.reshape(current.shape[0], feature_width)
    mixed_rows = (1.0 - restart) * summed + restart * start_rows.astype(jnp.float32)
    mixed_low = mixed_rows.astype(jnp.bfloat16)
    factor = math.log(strength / layer_number + 1.0)
    product = jnp.dot(mixed_low, weight, preferred_element_type=jnp.float32)
    inner_sum = (1.0 - factor) * mixed_rows + factor * product
    return jnp.maximum(inner_sum, 0.0).astype(jnp.bfloat16), mixed_low


def reference(h_zero, h_prev, hist_a, hist_b, tile_vals, tile_cols, pull_rows, pull_counts, weight_two, weight_three, grad_out):
    shard_a = hist_a.reshape(N_DEV, SHARD, WIDTH)
    shard_b = hist_b.reshape(N_DEV, SHARD, WIDTH)
    owners = jnp.arange(N_DEV, dtype=jnp.int32)[:, None]
    slot_ids = jnp.arange(TILE, dtype=jnp.int32)[None, :]

    def device(items):
        worker, start_rows, current, values, columns, wanted, counts, upstream = items
        home_shard = (worker // N_REP).astype(jnp.int32)
        live_mask = (slot_ids < counts[:, None])[:, :, None]
        pulled_a = jnp.where(live_mask, shard_a[owners, wanted], jnp.zeros((), shard_a.dtype))
        pulled_b = jnp.where(live_mask, shard_b[owners, wanted], jnp.zeros((), shard_b.dtype))
        own_a = lax.dynamic_index_in_dim(shard_a, home_shard, 0, keepdims=False)
        own_b = lax.dynamic_index_in_dim(shard_b, home_shard, 0, keepdims=False)
        second, unused_mix = propagate(current, own_a, pulled_a, values, columns, start_rows, weight_two, 2)
        layer_out, mixed_low = propagate(second, own_b, pulled_b, values, columns, start_rows, weight_three, 3)
        factor = math.log(strength / 3 + 1.0)
        grad_term = factor * jnp.dot(mixed_low.T, upstream, preferred_element_type=jnp.float32)
        return layer_out, second, grad_term

    items = (
        jnp.arange(WORKERS, dtype=jnp.int32),
        h_zero.reshape(WORKERS, BATCH, WIDTH),
        h_prev.reshape(WORKERS, BATCH, WIDTH),
        tile_vals.reshape(WORKERS, ROWBLK, TPR, TILE, TILE),
        tile_cols.reshape(WORKERS, ROWBLK, TPR),
        pull_rows,
        pull_counts,
        grad_out.reshape(WORKERS, BATCH, WIDTH),
    )
    layer_out, second, grad_terms = lax.map(device, items)
    return layer_out.reshape(NODES, WIDTH), second.reshape(NODES, WIDTH), jnp.sum(grad_terms, axis=0)
```

```python
import functools
import math

import jax
import jax.numpy as jnp
from jax import lax
from jax.experimental import pallas as pl
from jax.experimental.pallas import tpu as pltpu
from jax.sharding import PartitionSpec as P

restart = 0.1
strength = 0.5
near_tiles = 4
most_permutes = 8


f32 = jnp.float32
bf16 = jnp.bfloat16
vmem = pl.BlockSpec(memory_space=pltpu.VMEM)
smem = pl.BlockSpec(memory_space=pltpu.SMEM)
anywhere = pl.BlockSpec(memory_space=pl.ANY)


def params(mebibytes):
    return pltpu.CompilerParams(vmem_limit_bytes=mebibytes * 1024 * 1024)


def serve_kernel(pos_ref, idx_ref, hist_ref, *rest, peers, slots, chunk, paired):
    outs, (shard, picks, acc, sems) = rest[:-4], rest[-4:]
    rows, width = shard.shape
    steps = rows // chunk

    def load(step):
        part = pl.ds(step * chunk, chunk)
        return pltpu.make_async_copy(hist_ref.at[part], shard.at[part], sems.at[step])

    for step in range(steps):
        load(step).start()
    pos = pos_ref[0]
    asked = [idx_ref[pl.ds(jnp.bitwise_xor(pos, k) if paired else k, 1), :] for k in range(peers)]
    for first in range(0, peers, 8):
        turned = jnp.transpose(jnp.concatenate(asked[first : first + 8], axis=0))
        for k in range(8):
            picks[pl.ds((first + k) * slots, slots), :] = jnp.broadcast_to(turned[:, k : k + 1], (slots, 128))
    lanes = lax.broadcasted_iota(jnp.int32, (slots, 128), 1)
    for step in range(steps):
        load(step).wait()
        table = shard[pl.ds(step * chunk, chunk), :]

        def block(k, carry, step=step, table=table):
            part = pl.ds(pl.multiple_of(k * slots, slots), slots)
            wanted = picks[part, :]
            hot = jnp.concatenate(
                [
                    jnp.where(wanted == lanes + (step * chunk + low), 1.0, 0.0).astype(bf16)
                    for low in range(0, chunk, 128)
                ],
                axis=1,
            )
            found = jnp.dot(hot, table, preferred_element_type=f32)
            acc[part, :] = found if step == 0 else acc[part, :] + found
            return carry

        lax.fori_loop(0, peers, block, 0, unroll=8)
    if paired:
        for k in range(peers):
            outs[k][...] = acc[pl.ds(k * slots, slots), :].astype(bf16)
    else:
        for k in range(peers):
            outs[0][k] = acc[pl.ds(k * slots, slots), :].astype(bf16)


def serve(pos, asked, history, paired):
    peers, slots = asked.shape
    rows, width = history.shape
    chunk = min(1024, rows)
    one = jax.ShapeDtypeStruct((slots, width), bf16)
    whole = jax.ShapeDtypeStruct((peers, slots, width), bf16)
    return pl.pallas_call(
        functools.partial(serve_kernel, peers=peers, slots=slots, chunk=chunk, paired=paired),
        out_shape=[one] * peers if paired else [whole],
        in_specs=[smem, vmem, anywhere],
        out_specs=[vmem] * (peers if paired else 1),
        scratch_shapes=[
            pltpu.VMEM((rows, width), bf16),
            pltpu.VMEM((peers * slots, 128), jnp.int32),
            pltpu.VMEM((peers * slots, width), f32),
            pltpu.SemaphoreType.DMA((rows // chunk,)),
        ],
        compiler_params=params(16 if peers <= 8 else 40),
        name="serve",
    )(pos, asked, history)


def gather_pulled(pos_ref, counts_ref, pulled, remote, paired):
    peers, slots, width = remote.shape
    slot_ids = lax.broadcasted_iota(jnp.int32, (slots, width), 0)
    for k in range(peers):
        owner = jnp.bitwise_xor(pos_ref[0], k) if paired else k
        block = pulled[k][...] if paired else pulled[0][k]
        live = slot_ids < counts_ref[0, owner]
        remote[owner] = jnp.where(live, block.astype(f32), 0.0).astype(bf16)


def beside(vals_ref, i, tiles):
    return jnp.concatenate([vals_ref[i, t] for t in tiles], axis=1)


def layer_a_kernel(
    pos_ref, cols_ref, counts_ref, vals_ref, current_ref, hist_a_ref, hist_b_ref, zero_ref, weight_ref,
    *rest, paired, n_pulled, factor,
):
    pulled = rest[:n_pulled]
    new_ref, pre_ref, ordered_ref = rest[n_pulled : n_pulled + 3]
    home_a, home_b, remote, sems = rest[n_pulled + 3 :]
    row_blocks, tiles, size, _ = vals_ref.shape
    peers = remote.shape[0]
    width = remote.shape[2]
    own = current_ref.shape[0] // size
    base = own + hist_a_ref.shape[0] // size
    homes = near_tiles - 1

    def copies(source, target, side):
        made = []
        for i in range(row_blocks):
            for t in range(homes):
                start = pl.multiple_of((cols_ref[i, 1 + t] - own) * size, size)
                made.append(
                    pltpu.make_async_copy(
                        source.at[pl.ds(start, size)], target.at[i * homes + t], sems.at[side, i * homes + t]
                    )
                )
        return made

    loads_a = copies(hist_a_ref, home_a, 0)
    loads_b = copies(hist_b_ref, home_b, 1)
    for load in loads_a + loads_b:
        load.start()
    gather_pulled(pos_ref, counts_ref, pulled, remote, paired)
    if paired:
        for i in range(row_blocks):
            for t in range(near_tiles, tiles):
                owner = cols_ref[i, t] - base
                ordered_ref[owner, pl.ds(i * size, size), :] = vals_ref[i, t]
        far = jnp.zeros((row_blocks * size, width), f32)
        for p in range(0, peers, 2):
            far += jnp.dot(
                jnp.concatenate([ordered_ref[p], ordered_ref[p + 1]], axis=1),
                remote[pl.ds(p, 2)].reshape(2 * size, width),
                preferred_element_type=f32,
            )
    for load in loads_a:
        load.wait()
    for i in range(row_blocks):
        rows = pl.ds(i * size, size)
        start = pl.multiple_of(cols_ref[i, 0] * size, size)
        sources = [current_ref[pl.ds(start, size), :]] + [home_a[i * homes + t] for t in range(homes)]
        summed = jnp.dot(beside(vals_ref, i, range(near_tiles)), jnp.concatenate(sources, axis=0), preferred_element_type=f32)
        if paired:
            summed += far[i * size : (i + 1) * size]
        else:
            blocks = [remote[cols_ref[i, t] - base] for t in range(near_tiles, tiles)]
            summed += jnp.dot(
                beside(vals_ref, i, range(near_tiles, tiles)), jnp.concatenate(blocks, axis=0), preferred_element_type=f32
            )
        mixed = (1.0 - restart) * summed + restart * zero_ref[rows, :].astype(f32)
        product = jnp.dot(mixed.astype(bf16), weight_ref[...], preferred_element_type=f32)
        new_ref[rows, :] = jnp.maximum((1.0 - factor) * mixed + factor * product, 0.0).astype(bf16)
    for load in loads_b:
        load.wait()
    for i in range(row_blocks):
        rows = pl.ds(i * size, size)
        start = pl.multiple_of(cols_ref[i, 0] * size, size)
        sources = [new_ref[pl.ds(start, size), :]] + [home_b[i * homes + t] for t in range(homes)]
        summed = jnp.dot(beside(vals_ref, i, range(near_tiles)), jnp.concatenate(sources, axis=0), preferred_element_type=f32)
        pre_ref[rows, :] = (1.0 - restart) * summed + restart * zero_ref[rows, :].astype(f32)
        if not paired:
            ordered_ref[i] = beside(vals_ref, i, range(near_tiles, tiles))


def layer_b_kernel(
    pos_ref, cols_ref, counts_ref, ordered_ref, pre_ref, upstream_ref, weight_ref, *rest, paired, n_pulled, factor, base,
):
    pulled = rest[:n_pulled]
    out_ref, grad_ref, remote, low_ref = rest[n_pulled:]
    peers, size, width = remote.shape
    rows_all = pre_ref.shape[0]
    gather_pulled(pos_ref, counts_ref, pulled, remote, paired)
    if paired:
        far = jnp.zeros((rows_all, width), f32)
        for p in range(0, peers, 2):
            far += jnp.dot(
                jnp.concatenate([ordered_ref[p], ordered_ref[p + 1]], axis=1),
                remote[pl.ds(p, 2)].reshape(2 * size, width),
                preferred_element_type=f32,
            )
    for i in range(rows_all // size):
        rows = pl.ds(i * size, size)
        if paired:
            summed = far[i * size : (i + 1) * size]
        else:
            blocks = [remote[cols_ref[i, t] - base] for t in range(near_tiles, cols_ref.shape[1])]
            summed = jnp.dot(ordered_ref[i], jnp.concatenate(blocks, axis=0), preferred_element_type=f32)
        mixed = (1.0 - restart) * summed + pre_ref[rows, :]
        low = mixed.astype(bf16)
        low_ref[rows, :] = low
        product = jnp.dot(low, weight_ref[...], preferred_element_type=f32)
        out_ref[rows, :] = jnp.maximum((1.0 - factor) * mixed + factor * product, 0.0).astype(bf16)
    grad_ref[...] = factor * lax.dot_general(
        low_ref[...], upstream_ref[...], (((0,), (0,)), ((), ())), preferred_element_type=f32
    )


def assemble_kernel(rep_ref, *rest):
    parts, out_ref, sems = rest[:-2], rest[-2], rest[-1]
    size = parts[0].shape[0]
    made = []
    for k, part in enumerate(parts):
        start = pl.multiple_of(jnp.bitwise_xor(rep_ref[0], k) * size, size)
        made.append(pltpu.make_async_copy(part, out_ref.at[pl.ds(start, size)], sems.at[k]))
        made[-1].start()
    for copy in made:
        copy.wait()


def swap(value, axis, count, mask):
    return lax.ppermute(value, axis, [(i, i ^ mask) for i in range(count)])


def local(
    h_zero, h_prev, hist_a, hist_b, tile_vals, tile_cols, pull_rows, pull_counts, weight_two, weight_three, grad_out,
    *, owners, replicas,
):
    row_blocks, tiles, size, _ = tile_vals.shape
    batch, width = h_prev.shape
    slots = pull_rows.shape[2]
    paired = owners <= most_permutes and owners == tiles - near_tiles and owners & (owners - 1) == 0
    n_pulled = owners if paired else 1
    pos = lax.axis_index("dev").astype(jnp.int32).reshape(1)
    asked = lax.all_to_all(pull_rows[0], "dev", split_axis=0, concat_axis=0, tiled=True)

    def exchange(history):
        blocks = serve(pos, asked, history, paired)
        if not paired:
            return [lax.all_to_all(blocks[0], "dev", split_axis=0, concat_axis=0, tiled=True)]
        moved = [blocks[0]] + [None] * (owners - 1)
        for k in list(range(owners // 2, owners)) + list(range(1, owners // 2)):
            moved[k] = swap(blocks[k], "dev", owners, k)
        return moved

    pulled_a = exchange(hist_a)
    pulled_b = exchange(hist_b)
    homes = row_blocks * (near_tiles - 1)
    remote_scratch = pltpu.VMEM((owners, slots, width), bf16)
    ordered_shape = (owners, batch, size) if paired else (row_blocks, size, (tiles - near_tiles) * size)
    second, pre, ordered = pl.pallas_call(
        functools.partial(layer_a_kernel, paired=paired, n_pulled=n_pulled, factor=math.log(strength / 2 + 1.0)),
        out_shape=[
            jax.ShapeDtypeStruct((batch, width), bf16),
            jax.ShapeDtypeStruct((batch, width), f32),
            jax.ShapeDtypeStruct(ordered_shape, bf16),
        ],
        in_specs=[smem] * 3 + [vmem] * 2 + [anywhere] * 2 + [vmem] * (2 + n_pulled),
        out_specs=[vmem] * 3,
        scratch_shapes=[
            pltpu.VMEM((homes, size, width), bf16),
            pltpu.VMEM((homes, size, width), bf16),
            remote_scratch,
            pltpu.SemaphoreType.DMA((2, homes)),
        ],
        compiler_params=params(32),
        name="layer_a",
    )(pos, tile_cols, pull_counts, tile_vals, h_prev, hist_a, hist_b, h_zero, weight_two, *pulled_a)

    layer_three, grad_term = pl.pallas_call(
        functools.partial(
            layer_b_kernel, paired=paired, n_pulled=n_pulled, factor=math.log(strength / 3 + 1.0),
            base=(batch + hist_a.shape[0]) // size,
        ),
        out_shape=[jax.ShapeDtypeStruct((batch, width), bf16), jax.ShapeDtypeStruct((width, width), f32)],
        in_specs=[smem] * 3 + [vmem] * (4 + n_pulled),
        out_specs=[vmem] * 2,
        scratch_shapes=[remote_scratch, pltpu.VMEM((batch, width), bf16)],
        compiler_params=params(24),
        name="layer_b",
    )(pos, tile_cols, pull_counts, ordered, pre, grad_out, weight_three, *pulled_b)

    if replicas == 4:
        rep = lax.axis_index("rep").astype(jnp.int32).reshape(1)
        beside_one = swap(second, "rep", replicas, 1)
        beside_two = swap(second, "rep", replicas, 2)
        beside_three = swap(beside_two, "rep", replicas, 1)
        fresh_rows = pl.pallas_call(
            assemble_kernel,
            out_shape=jax.ShapeDtypeStruct((replicas * batch, width), bf16),
            in_specs=[smem] + [anywhere] * 4,
            out_specs=anywhere,
            scratch_shapes=[pltpu.SemaphoreType.DMA((4,))],
            compiler_params=params(1),
            name="assemble",
        )(rep, second, beside_one, beside_two, beside_three)
    else:
        fresh_rows = lax.all_gather(second, "rep", axis=0, tiled=True)

    both = ("dev", "rep")
    devices = owners * replicas
    if width % (8 * devices) == 0:
        share = lax.all_to_all(
            grad_term.reshape(devices, width // devices, width), both, split_axis=0, concat_axis=0, tiled=True
        )
        total = jnp.sum(share, axis=0).astype(bf16)
        spread = lax.all_to_all(
            jnp.broadcast_to(total[None], (devices,) + total.shape), both, split_axis=0, concat_axis=0, tiled=True
        )
        grad_total = spread.reshape(width, width).astype(f32)
    else:
        grad_total = lax.psum(grad_term, both)
    return (layer_three, fresh_rows, grad_total)


def solution(mesh):
    rows = P(("dev", "rep"), None)
    return jax.shard_map(
        functools.partial(local, owners=mesh.shape["dev"], replicas=mesh.shape["rep"]),
        mesh=mesh,
        in_specs=(
            rows, rows, P("dev", None), P("dev", None), P(("dev", "rep"), None, None, None), rows,
            P(("dev", "rep"), None, None), rows, P(), P(), rows,
        ),
        out_specs=(rows, P("dev", None), P()),
        check_vma=False,
    )
```

```python
import functools
import math

import jax
import jax.numpy as jnp
from jax import lax
from jax.experimental import pallas as pl
from jax.experimental.pallas import tpu as pltpu
from jax.sharding import PartitionSpec as P

restart = 0.1
strength = 0.5
near_tiles = 4
most_permutes = 8


f32 = jnp.float32
bf16 = jnp.bfloat16
vmem = pl.BlockSpec(memory_space=pltpu.VMEM)
smem = pl.BlockSpec(memory_space=pltpu.SMEM)
anywhere = pl.BlockSpec(memory_space=pl.ANY)
hbm = pl.BlockSpec(memory_space=pltpu.HBM)


def params(mebibytes):
    return pltpu.CompilerParams(vmem_limit_bytes=mebibytes * 1024 * 1024)


def in_hbm(value):
    return pltpu.with_memory_space_constraint(value, pltpu.HBM)


def rank3(value):
    return [value[:, low : low + 128] for low in range(0, value.shape[1], 128)]


def fetch_kernel(hist_a_ref, hist_b_ref, held_a_ref, held_b_ref, sems):
    copies = [
        pltpu.make_async_copy(hist_a_ref, held_a_ref, sems.at[0]),
        pltpu.make_async_copy(hist_b_ref.at[pl.ds(0, held_b_ref.shape[0])], held_b_ref, sems.at[1]),
    ]
    for copy in copies:
        copy.start()
    for copy in copies:
        copy.wait()


def fetch(hist_a, hist_b):
    rows, width = hist_a.shape
    return pl.pallas_call(
        fetch_kernel,
        out_shape=[pltpu.VMEM((rows, width), bf16), pltpu.VMEM((rows * 5 // 8, width), bf16)],
        in_specs=[hbm] * 2,
        out_specs=[vmem] * 2,
        scratch_shapes=[pltpu.SemaphoreType.DMA((2,))],
        compiler_params=params(1),
        name="fetch",
    )(in_hbm(hist_a), in_hbm(hist_b))


def serve_kernel(pos_ref, idx_ref, held_a_ref, held_b_ref, hist_b_ref, *rest, peers, slots, paired):
    outs, (tail, table, found, sem) = rest[:-4], rest[-4:]
    rows, width = held_a_ref.shape
    head = rows - tail.shape[0]
    unroll = 16
    load = pltpu.make_async_copy(hist_b_ref.at[pl.ds(head, rows - head)], tail, sem)
    load.start()
    for at, piece in enumerate(rank3(held_a_ref[...])):
        table[:, at, :] = piece.astype(f32)
    for at, piece in enumerate(rank3(held_b_ref[...])):
        table[pl.ds(0, head), width // 128 + at, :] = piece.astype(f32)
    load.wait()
    for at, piece in enumerate(rank3(tail[...])):
        table[pl.ds(head, rows - head), width // 128 + at, :] = piece.astype(f32)
    for k in range(peers):
        peer = jnp.bitwise_xor(pos_ref[0], k) if paired else k

        def pick(j, carry, k=k, peer=peer):
            for u in range(unroll):
                slot = j * unroll + u
                found[k * slots + slot] = table[idx_ref[peer, slot]]
            return carry

        lax.fori_loop(0, slots // unroll, pick, 0)
        part = pl.ds(k * slots, slots)
        for at in range(table.shape[1]):
            half, low = divmod(at * 128, width)
            piece = found[part, at, :].astype(bf16)
            if paired:
                outs[k][pl.ds(half * slots, slots), pl.ds(low, 128)] = piece
            else:
                outs[0][k, pl.ds(half * slots, slots), pl.ds(low, 128)] = piece


def serve(pos, asked, held_a, held_b, hist_b, paired):
    peers, slots = asked.shape
    rows, width = held_a.shape
    pieces = 2 * width // 128
    one = jax.ShapeDtypeStruct((2 * slots, width), bf16)
    whole = jax.ShapeDtypeStruct((peers, 2 * slots, width), bf16)
    return pl.pallas_call(
        functools.partial(serve_kernel, peers=peers, slots=slots, paired=paired),
        out_shape=[one] * peers if paired else [whole],
        in_specs=[smem, smem, vmem, vmem, hbm],
        out_specs=[vmem] * (peers if paired else 1),
        scratch_shapes=[
            pltpu.VMEM((rows - held_b.shape[0], width), bf16),
            pltpu.VMEM((rows, pieces, 128), f32),
            pltpu.VMEM((peers * slots, pieces, 128), f32),
            pltpu.SemaphoreType.DMA,
        ],
        compiler_params=params(20 if paired else 48),
        name="serve",
    )(pos, asked, held_a, held_b, in_hbm(hist_b))


def beside(vals_ref, i, tiles):
    return jnp.concatenate([vals_ref[i, t] for t in tiles], axis=1)


def near_kernel(
    cols_ref, vals_ref, current_ref, hist_a_ref, hist_b_ref, zero_ref, after_ref,
    near_a_ref, near_b_ref, far_tiles_ref, own_tiles_ref, vals, home_a, home_b, sems, *, paired,
):
    row_blocks, tiles, size, _ = vals.shape
    own = current_ref.shape[0] // size
    base = own + hist_a_ref.shape[0] // size
    homes = near_tiles - 1
    load_vals = [pltpu.make_async_copy(vals_ref.at[i], vals.at[i], sems.at[2, i]) for i in range(row_blocks)]
    loads = []
    for i in range(row_blocks):
        for side, (source, target) in enumerate(((hist_a_ref, home_a), (hist_b_ref, home_b))):
            for t in range(homes):
                start = pl.multiple_of((cols_ref[i, 1 + t] - own) * size, size)
                at = i * homes + t
                loads.append(
                    pltpu.make_async_copy(source.at[pl.ds(start, size)], target.at[pl.ds(at * size, size)], sems.at[side, at])
                )
    for i in range(row_blocks):
        load_vals[i].start()
        for load in loads[2 * homes * i : 2 * homes * (i + 1)]:
            load.start()
    for i in range(row_blocks):
        rows = pl.ds(i * size, size)
        load_vals[i].wait()
        for t in range(near_tiles, tiles):
            place = cols_ref[i, t] - base if paired else t - near_tiles
            far_tiles_ref[rows, pl.ds(pl.multiple_of(place * size, size), size)] = vals[i, t]
        own_tiles_ref[i] = vals[i, 0]
        for load in loads[2 * homes * i : 2 * homes * (i + 1)]:
            load.wait()
        start = pl.multiple_of(cols_ref[i, 0] * size, size)
        home_rows = pl.ds(i * homes * size, homes * size)
        source = jnp.concatenate([current_ref[pl.ds(start, size), :], home_a[home_rows, :]], axis=0)
        initial = restart * zero_ref[rows, :].astype(f32)
        near_a_ref[rows, :] = (1.0 - restart) * jnp.dot(
            beside(vals, i, range(near_tiles)), source, preferred_element_type=f32
        ) + initial
        near_b_ref[rows, :] = (1.0 - restart) * jnp.dot(
            beside(vals, i, range(1, near_tiles)), home_b[home_rows, :], preferred_element_type=f32
        ) + initial


def layers_kernel(
    pos_ref, cols_ref, counts_ref, far_tiles_ref, own_tiles_ref, near_a_ref, near_b_ref, weight_two_ref,
    weight_three_ref, upstream_ref, *rest, paired, n_pulled, base, factor_two, factor_three,
):
    pulled = rest[:n_pulled]
    new_ref, out_ref, grad_ref, remote, low_ref, far_ref = rest[n_pulled:]
    peers, slots = counts_ref.shape[1], remote.shape[0] // counts_ref.shape[1]
    row_blocks, size, _ = own_tiles_ref.shape
    width = near_a_ref.shape[1]
    slot_ids = lax.broadcasted_iota(jnp.int32, (slots, width), 0)
    for k in range(peers):
        owner = jnp.bitwise_xor(pos_ref[0], k) if paired else k
        block = pulled[k] if paired else pulled[0].at[k]
        live = slot_ids < counts_ref[0, owner]
        rows = pl.ds(pl.multiple_of(owner * slots, slots), slots)
        for half in range(2):
            kept = jnp.where(live, block[pl.ds(half * slots, slots), :].astype(f32), 0.0).astype(bf16)
            remote[rows, pl.ds(half * width, width)] = kept
    if paired:
        far_ref[...] = jnp.dot(far_tiles_ref[...], remote[...], preferred_element_type=f32)
    else:
        for i in range(row_blocks):
            rows = pl.ds(i * size, size)
            blocks = [
                remote[pl.ds(pl.multiple_of((cols_ref[i, t] - base) * slots, slots), slots), :]
                for t in range(near_tiles, cols_ref.shape[1])
            ]
            far_ref[rows, :] = jnp.dot(
                far_tiles_ref[rows, :], jnp.concatenate(blocks, axis=0), preferred_element_type=f32
            )
    mixed = (1.0 - restart) * far_ref[:, pl.ds(0, width)] + near_a_ref[...]
    product = jnp.dot(mixed.astype(bf16), weight_two_ref[...], preferred_element_type=f32)
    new_ref[...] = jnp.maximum((1.0 - factor_two) * mixed + factor_two * product, 0.0).astype(bf16)
    for i in range(row_blocks):
        rows = pl.ds(i * size, size)
        start = pl.multiple_of(cols_ref[i, 0] * size, size)
        summed = far_ref[rows, pl.ds(width, width)] + jnp.dot(
            own_tiles_ref[i], new_ref[pl.ds(start, size), :], preferred_element_type=f32
        )
        mixed = (1.0 - restart) * summed + near_b_ref[rows, :]
        low = mixed.astype(bf16)
        low_ref[rows, :] = low
        product = jnp.dot(low, weight_three_ref[...], preferred_element_type=f32)
        out_ref[rows, :] = jnp.maximum((1.0 - factor_three) * mixed + factor_three * product, 0.0).astype(bf16)
    grad_ref[...] = factor_three * lax.dot_general(
        low_ref[...], upstream_ref[...], (((0,), (0,)), ((), ())), preferred_element_type=f32
    )


def assemble_kernel(rep_ref, *rest):
    parts, out_ref, sems = rest[:-2], rest[-2], rest[-1]
    size = parts[0].shape[0]
    made = []
    for k, part in enumerate(parts):
        start = pl.multiple_of(jnp.bitwise_xor(rep_ref[0], k) * size, size)
        made.append(pltpu.make_async_copy(part, out_ref.at[pl.ds(start, size)], sems.at[k]))
        made[-1].start()
    for copy in made:
        copy.wait()


def swap(value, axis, count, mask):
    return lax.ppermute(value, axis, [(i, i ^ mask) for i in range(count)])


def local(
    h_zero, h_prev, hist_a, hist_b, tile_vals, tile_cols, pull_rows, pull_counts, weight_two, weight_three, grad_out,
    *, owners, replicas,
):
    row_blocks, tiles, size, _ = tile_vals.shape
    batch, width = h_prev.shape
    slots = pull_rows.shape[2]
    paired = owners <= most_permutes and owners == tiles - near_tiles and owners & (owners - 1) == 0
    n_pulled = owners if paired else 1
    pos = lax.axis_index("dev").astype(jnp.int32).reshape(1)
    asked = lax.all_to_all(pull_rows[0], "dev", split_axis=0, concat_axis=0, tiled=True)
    held_a, held_b = fetch(hist_a, hist_b)
    blocks = serve(pos, asked, held_a, held_b, hist_b, paired)
    if paired:
        pulled = [blocks[0]] + [None] * (owners - 1)
        for k in list(range(owners // 2, owners)) + list(range(1, owners // 2)):
            pulled[k] = swap(blocks[k], "dev", owners, k)
    else:
        pulled = [lax.all_to_all(blocks[0], "dev", split_axis=0, concat_axis=0, tiled=True)]
    homes = row_blocks * (near_tiles - 1)
    far_tiles = tiles - near_tiles
    near_a, near_b, far, own = pl.pallas_call(
        functools.partial(near_kernel, paired=paired),
        out_shape=[
            jax.ShapeDtypeStruct((batch, width), f32),
            jax.ShapeDtypeStruct((batch, width), f32),
            jax.ShapeDtypeStruct((batch, far_tiles * size), bf16),
            jax.ShapeDtypeStruct((row_blocks, size, size), bf16),
        ],
        in_specs=[smem, hbm, vmem, hbm, hbm, vmem, anywhere],
        out_specs=[vmem] * 4,
        scratch_shapes=[
            pltpu.VMEM(tile_vals.shape, bf16),
            pltpu.VMEM((homes * size, width), bf16),
            pltpu.VMEM((homes * size, width), bf16),
            pltpu.SemaphoreType.DMA((3, homes)),
        ],
        compiler_params=params(20),
        name="near",
    )(tile_cols, in_hbm(tile_vals), h_prev, in_hbm(hist_a), in_hbm(hist_b), h_zero, blocks[0])
    second, layer_three, grad_term = pl.pallas_call(
        functools.partial(
            layers_kernel, paired=paired, n_pulled=n_pulled, base=(batch + hist_a.shape[0]) // size,
            factor_two=math.log(strength / 2 + 1.0), factor_three=math.log(strength / 3 + 1.0),
        ),
        out_shape=[
            jax.ShapeDtypeStruct((batch, width), bf16),
            jax.ShapeDtypeStruct((batch, width), bf16),
            jax.ShapeDtypeStruct((width, width), f32),
        ],
        in_specs=[smem] * 3 + [vmem] * (7 + n_pulled),
        out_specs=[vmem] * 3,
        scratch_shapes=[
            pltpu.VMEM((owners * slots, 2 * width), bf16),
            pltpu.VMEM((batch, width), bf16),
            pltpu.VMEM((batch, 2 * width), f32),
        ],
        compiler_params=params(24 if paired else 48),
        name="layers",
    )(pos, tile_cols, pull_counts, far, own, near_a, near_b, weight_two, weight_three, grad_out, *pulled)

    if replicas == 4:
        rep = lax.axis_index("rep").astype(jnp.int32).reshape(1)
        beside_one = swap(second, "rep", replicas, 1)
        beside_two = swap(second, "rep", replicas, 2)
        beside_three = swap(beside_two, "rep", replicas, 1)
        fresh_rows = pl.pallas_call(
            assemble_kernel,
            out_shape=jax.ShapeDtypeStruct((replicas * batch, width), bf16),
            in_specs=[smem] + [anywhere] * 4,
            out_specs=anywhere,
            scratch_shapes=[pltpu.SemaphoreType.DMA((4,))],
            compiler_params=params(1),
            name="assemble",
        )(rep, second, beside_one, beside_two, beside_three)
    else:
        fresh_rows = lax.all_gather(second, "rep", axis=0, tiled=True)

    both = ("dev", "rep")
    devices = owners * replicas
    if width % (8 * devices) == 0:
        share = lax.all_to_all(
            grad_term.reshape(devices, width // devices, width), both, split_axis=0, concat_axis=0, tiled=True
        )
        total = jnp.sum(share, axis=0).astype(bf16)
        spread = lax.all_to_all(
            jnp.broadcast_to(total[None], (devices,) + total.shape), both, split_axis=0, concat_axis=0, tiled=True
        )
        grad_total = spread.reshape(width, width).astype(f32)
    else:
        grad_total = lax.psum(grad_term, both)
    return (layer_three, fresh_rows, grad_total)


def solution(mesh):
    rows = P(("dev", "rep"), None)
    return jax.shard_map(
        functools.partial(local, owners=mesh.shape["dev"], replicas=mesh.shape["rep"]),
        mesh=mesh,
        in_specs=(
            rows, rows, P("dev", None), P("dev", None), P(("dev", "rep"), None, None, None), rows,
            P(("dev", "rep"), None, None), rows, P(), P(), rows,
        ),
        out_specs=(rows, P("dev", None), P()),
        check_vma=False,
    )
```
